32 devices in a mesh: dp: 8 (over z, x), mp: 4 (over y, core).
Axes of the slice: x: 2, y: 2, z: 4, core: 2. Of those that a mesh axis runs over, the one named last changes fastest.
Arguments:
- q_latent: bfloat16 [2048, 2, 768], P('dp', None, 'mp'), may hold values from -6 to 6
- kv_latent: bfloat16 [2048, 2, 256], P('dp', None, 'mp'), may hold values from -6 to 6
- q_head_grad: bfloat16 [2048, 512], P('dp'), may hold values from -0.1875 to 0.1875
- k_head_grad: bfloat16 [2048, 512], P('dp'), may hold values from -0.1875 to 0.1875
- q_heads: bfloat16 [2048, 512], P('dp', 'mp'), may hold values from -6 to 6
- k_heads: bfloat16 [2048, 512], P('dp', 'mp'), may hold values from -6 to 6
- query_pick: int32 [8, 16, 4], P('dp', None, 'mp'), may hold values from 0 to 255
- key_pick: int32 [8, 16, 4], P('dp', None, 'mp'), may hold values from 0 to 255
- q_weight: float32 [8, 768, 128], P('dp', 'mp'), may hold values from -6 to 6
- k_weight: float32 [8, 256, 128], P('dp', 'mp'), may hold values from -6 to 6
- q_moment: float32 [8, 768, 128], P('dp', 'mp'), may hold values from -6 to 6
- k_moment: float32 [8, 256, 128], P('dp', 'mp'), may hold values from -6 to 6
Outputs:
- q_weight_new: float32 [8, 768, 128], P('dp', 'mp')
- k_weight_new: float32 [8, 256, 128], P('dp', 'mp')
- q_moment_new: float32 [8, 768, 128], P('dp', 'mp')
- k_moment_new: float32 [8, 256, 128], P('dp', 'mp')
The draws below stay inside these ranges and needn't reach their ends.
Inputs may be any that keep to these rules, and one draw needn't show every extreme that they name: `query_pick`: the index of a token among the 256 tokens of its own block b. `key_pick`: the index of a token among the 256 tokens of its own block b.
All inputs are finite; a program needn't handle non-finite values.
Results may differ from the reference program's by a relative error of at most 0.0003.
Values sent between devices are 32-bit elements; how exact they have to be, the bound alone decides.
A program may use at most 64 MiB of HBM per device.

```python
import math
import jax
import jax.numpy as jnp
from jax import lax

QR = 1536
KR = 512
DN = 128
TOK_DEV = 256
PICKS = 16
ITERS = 5
HEADS = 4
TOKENS = 2048
N_DP = 8


def touch_ends(result, stream_key, low, top_value):
    dims = result.shape
    spot = [jax.random.randint(jax.random.fold_in(stream_key, axis), (), 0, dims[axis]) for axis in range(len(dims))]
    result = result.at[tuple(spot)].set(low)
    longest = dims.index(max(dims))
    spot[longest] = (spot[longest] + 1) % dims[longest]
    return result.at[tuple(spot)].set(top_value)


def strengthened(result, stream_key, source, target, parts, factor):
    owner, partner = [(jnp.arange(result.shape[axis_at]) // (result.shape[axis_at] // parts)).reshape([-1 if axis == axis_at else 1 for axis in range(result.ndim)]) for axis_at in (source, target)]
    chosen = jax.random.permutation(stream_key, parts)[partner]
    strong = (owner == chosen) | (owner == (partner + parts // 2) % parts)
    return jnp.where(strong, factor * result, result)


def levels(key, dims, pieces, low, high):
    def one(position, shards_of):
        steps = jax.random.uniform(jax.random.fold_in(jax.random.fold_in(key, 6), position), (shards_of,), jnp.float32, low / len(pieces), high / len(pieces))
        return jnp.repeat(jnp.exp(steps), dims[position] // shards_of).reshape((-1,) + (1,) * (len(dims) - position - 1))

    loudness = one(*pieces[0])
    for cut in pieces[1:]:
        loudness = loudness * one(*cut)
    return loudness


def gaussian(own_key, extent, spread, bound, cuts=(), kind=jnp.bfloat16):
    result = spread * jax.random.normal(own_key, extent, jnp.float32)
    if cuts:
        result = result * levels(own_key, extent, cuts, -0.22, 0.18)
    return jnp.clip(result, -bound, bound).astype(kind)


def bell_draw_with(rng, dims, scale, limit, shards, heavy, held_as=jnp.bfloat16):
    entries = scale * jax.random.normal(rng, dims, jnp.float32)
    if shards:
        entries = entries * levels(rng, dims, shards, -0.22, 0.18)
    return jnp.clip(strengthened(entries, jax.random.fold_in(rng, 3), *heavy), -limit, limit).astype(held_as)


def setup_inputs(seed: int = 0) -> dict:
    key_list = jax.random.split(jax.random.key(seed), 13)
    return {
        "q_latent": gaussian(key_list[0], (TOKENS, 2, QR // 2), 1.0, 6.0, ((0, 8), (2, 4))),
        "kv_latent": gaussian(key_list[1], (TOKENS, 2, KR // 2), 1.0, 6.0, ((0, 8), (2, 4))),
        "q_head_grad": bell_draw_with(key_list[2], (TOKENS, HEADS * DN), TOKENS ** -0.5, 0.1875, ((0, 8),), (0, 1, 8, 2.0)),
        "k_head_grad": bell_draw_with(key_list[3], (TOKENS, HEADS * DN), TOKENS ** -0.5, 0.1875, ((0, 8),), (0, 1, 8, 2.0)),
        "q_heads": gaussian(key_list[4], (TOKENS, HEADS * DN), 1.0, 6.0, ((0, 8), (1, 4))),
        "k_heads": gaussian(key_list[5], (TOKENS, HEADS * DN), 1.0, 6.0, ((0, 8), (1, 4))),
        "query_pick": touch_ends(jax.random.randint(key_list[6], (N_DP, PICKS, HEADS), 0, TOK_DEV), jax.random.fold_in(key_list[6], 1), 0, TOK_DEV - 1).astype(jnp.int32),
        "key_pick": touch_ends(jax.random.randint(key_list[7], (N_DP, PICKS, HEADS), 0, TOK_DEV), jax.random.fold_in(key_list[7], 1), 0, TOK_DEV - 1).astype(jnp.int32),
        "q_weight": gaussian(key_list[8], (2 * HEADS, QR // 2, DN), 1.0, 6.0, ((0, 8), (1, 4)), jnp.float32),
        "k_weight": gaussian(key_list[9], (2 * HEADS, KR // 2, DN), 1.0, 6.0, ((0, 8), (1, 4)), jnp.float32),
        "q_moment": gaussian(key_list[10], (2 * HEADS, QR // 2, DN), 1.0, 6.0, ((0, 8), (1, 4)), jnp.float32),
        "k_moment": gaussian(key_list[11], (2 * HEADS, KR // 2, DN), 1.0, 6.0, ((0, 8), (1, 4)), jnp.float32),
    }


MOMENTUM = 0.95
STEP_SIZE = 1.0
DECAY = 0.1
CLIP_LEVEL = 0.1
SCORE_SCALE = 1.0 / math.sqrt(192.0)
COEFF_A = 3.4445
COEFF_B = -4.775
COEFF_C = 2.0315
HIGHEST = lax.Precision.HIGHEST

def grad_slots(latent, head_grad):
    flat = latent.reshape(latent.shape[0], -1)
    total = jnp.dot(flat.T, head_grad, preferred_element_type=jnp.float32)
    rows_all = total.shape[0]
    total = total.reshape(2, rows_all // 2, HEADS, DN).transpose(0, 2, 1, 3)
    return total.reshape(2 * HEADS, rows_all // 2, DN)

def to_heads(slots):
    count, half_rows, width = slots.shape
    stacked = slots.reshape(2, count // 2, half_rows, width).transpose(1, 0, 2, 3)
    return stacked.reshape(count // 2, 2 * half_rows, width)

def to_slots(stacked):
    heads, rows_all, width = stacked.shape
    split = stacked.reshape(heads, 2, rows_all // 2, width).transpose(1, 0, 2, 3)
    return split.reshape(2 * heads, rows_all // 2, width)

def gramians(stacked):
    return jnp.einsum('hrc,hrd->hcd', stacked, stacked, precision=HIGHEST)

def polar(stacked):
    grams = gramians(stacked)
    scale = 1.0 / jnp.sqrt(jnp.trace(grams, axis1=1, axis2=2) + 1.0)
    current = stacked * scale[:, None, None]
    grams = grams * (scale * scale)[:, None, None]
    for step in range(ITERS):
        square = jnp.einsum('hcd,hde->hce', grams, grams, precision=HIGHEST)
        mixer = COEFF_B * grams + COEFF_C * square
        current = COEFF_A * current + jnp.einsum('hrc,hcd->hrd', current, mixer, precision=HIGHEST)
        if step + 1 < ITERS:
            grams = gramians(current)
    return current

def head_peaks(q_heads, k_heads, query_pick, key_pick):
    q_cube = q_heads.reshape(N_DP, TOK_DEV, HEADS, DN)
    k_cube = k_heads.reshape(N_DP, TOK_DEV, HEADS, DN)
    picked_q = jnp.take_along_axis(q_cube, query_pick.astype(jnp.int32)[..., None], axis=1)
    picked_k = jnp.take_along_axis(k_cube, key_pick.astype(jnp.int32)[..., None], axis=1)
    scores = lax.optimization_barrier(jnp.sum(picked_q.astype(jnp.float32) * picked_k.astype(jnp.float32), axis=3)) * SCORE_SCALE
    return lax.optimization_barrier(jnp.max(scores, axis=(0, 1)))

def reference(q_latent, kv_latent, q_head_grad, k_head_grad, q_heads, k_heads, query_pick, key_pick, q_weight, k_weight, q_moment, k_moment):
    q_moment_new = MOMENTUM * q_moment + grad_slots(q_latent, q_head_grad)
    k_moment_new = MOMENTUM * k_moment + grad_slots(kv_latent, k_head_grad)
    q_ortho = to_slots(polar(to_heads(q_moment_new)))
    k_ortho = to_slots(polar(to_heads(k_moment_new)))
    peak = head_peaks(q_heads, k_heads, query_pick, key_pick)
    shrink = jnp.sqrt(CLIP_LEVEL / jnp.maximum(peak, CLIP_LEVEL))
    shrink_slots = jnp.concatenate([shrink, shrink])[:, None, None]
    keep = 1.0 - STEP_SIZE * DECAY
    q_weight_new = (q_weight * keep - STEP_SIZE * 0.2 * math.sqrt(QR) * q_ortho) * shrink_slots
    k_weight_new = (k_weight * keep - STEP_SIZE * 0.2 * math.sqrt(KR) * k_ortho) * shrink_slots
    return (q_weight_new, k_weight_new, q_moment_new, k_moment_new)
```

```python
import functools
import math

import jax
import jax.numpy as jnp
from jax import lax
from jax.experimental import pallas as pl
from jax.experimental.pallas import tpu as pltpu
from jax.sharding import PartitionSpec as P

ITERS = 5
MOMENTUM = 0.95
STEP_SIZE = 1.0
DECAY = 0.1
CLIP_LEVEL = 0.1
SCORE_SCALE = 1.0 / math.sqrt(192.0)
COEFF_A = 3.4445
COEFF_B = -4.775
COEFF_C = 2.0315
LOWEST = -1e30
MESH = pl.DeviceIdType.MESH
F32 = jnp.float32
BF16 = jnp.bfloat16


def split(value):
    high = value.astype(BF16)
    return high, (value - high.astype(F32)).astype(BF16)


def mm(a, b):
    return jnp.dot(a, b, preferred_element_type=F32)


def mm3(a, b):
    return mm(a[0], b[0]) + (mm(a[0], b[1]) + mm(a[1], b[0]))


def gram(rows):
    high, low = split(rows)
    high_t = high.T
    cross = mm(high_t, low)
    return mm(high_t, high) + (cross + cross.T)


def partner(index, count, step):
    if count & (count - 1):
        return lax.rem(index + step, count)
    result = 0
    bit = 1
    while bit < count:
        held = lax.rem(lax.div(index, bit), 2)
        result = result + bit * ((1 - held) if step & bit else held)
        bit *= 2
    return result


def kernel(
    n_dp, n_mp, heads,
    lat_ref, qg_ref, kg_ref, qh_ref, kh_ref, qp_ref, kp_ref, qw_ref, kw_ref, qm_ref, km_ref,
    qw_out, kw_out, qm_out, km_out,
    near_send, near_recv, own, far_recv, peak_send, peak_recv, peak2_send, peak2_recv,
    grams, gram_recv, row_send, row_recv, z_send, z_recv, mix,
    ns_s, ns_r, fs_s, fs_r, pk_s, pk_r, pm_s, pm_r, g_s, g_r, y_s, y_r, z_s, z_r, m_s, m_r,
):
    dp = lax.axis_index("dp")
    mp = lax.axis_index("mp")
    n_outer = n_dp // 2
    outer = lax.div(dp, 2)
    inner = lax.rem(dp, 2)
    core = lax.rem(mp, 2)
    group = lax.div(mp, 2)
    n_group = n_mp // 2
    q_rows = qm_ref.shape[1]
    k_rows = km_ref.shape[1]
    width = qm_ref.shape[2]
    tokens = qg_ref.shape[0]
    other_core = mp + 1 - 2 * core

    barrier = pltpu.get_barrier_semaphore()
    for step in range(1, n_dp):
        pl.semaphore_signal(
            barrier, inc=1, device_id=(lax.rem(dp + step, n_dp), mp), device_id_type=MESH
        )
    for step in range(1, n_mp):
        pl.semaphore_signal(
            barrier, inc=1, device_id=(dp, lax.rem(mp + step, n_mp)), device_id_type=MESH
        )

    def copy(src, dst, send, recv, where):
        return pltpu.make_async_remote_copy(
            src_ref=src, dst_ref=dst, send_sem=send, recv_sem=recv,
            device_id=where, device_id_type=MESH,
        )

    def term(dst, where, to_outer, to_inner):
        slot = 2 * to_outer + to_inner
        half = lax.div(slot, heads)
        cols = pl.ds(pl.multiple_of(lax.rem(slot, heads) * width, width), width)
        dst[where, :q_rows, :] = mm(lat_ref[half, :q_rows, :], qg_ref[:, cols])
        dst[where, q_rows:, :] = mm(lat_ref[half, q_rows:, :], kg_ref[:, cols])

    order = list(range(n_outer - 1, -1, -1))
    neighbour = (dp + 1 - 2 * inner, mp)
    near = []
    for spot, step in enumerate(order):
        term(near_send, spot, partner(outer, n_outer, step), 1 - inner)
        if spot == 0:
            pl.semaphore_wait(barrier, n_dp + n_mp - 2)
        each = copy(near_send.at[spot], near_recv.at[spot], ns_s.at[spot], ns_r.at[spot], neighbour)
        each.start()
        near.append(each)

    local_heads = qp_ref.shape[2]
    lane = lax.broadcasted_iota(jnp.int32, (8, width), 1)
    peaks = jnp.full((8, width), LOWEST, F32)
    ids = lax.broadcasted_iota(jnp.int32, (qp_ref.shape[1], tokens), 1)
    for head in range(local_heads):
        span = slice(head * width, (head + 1) * width)
        pick_q = (ids == qp_ref[0, :, head : head + 1]).astype(F32).astype(BF16)
        pick_k = (ids == kp_ref[0, :, head : head + 1]).astype(F32).astype(BF16)
        score = jnp.sum(
            mm(pick_q, qh_ref[:, span]) * mm(pick_k, kh_ref[:, span]), axis=1, keepdims=True
        )
        top = jnp.max(score * SCORE_SCALE, axis=0, keepdims=True)
        peaks = jnp.where(lane == mp * local_heads + head, top, peaks)
    peak_send[...] = peaks
    peak_copies = []
    for step in range(1, n_dp):
        each = copy(
            peak_send, peak_recv.at[step - 1], pk_s.at[step - 1], pk_r.at[step - 1],
            (lax.rem(dp + step, n_dp), mp),
        )
        each.start()
        peak_copies.append(each)

    for spot, step in enumerate(order):
        term(own, spot, partner(outer, n_outer, step), inner)
    far = []
    for spot, step in enumerate(order):
        near[spot].wait_recv()
        if step:
            own[spot] = own[spot] + near_recv[spot]
            each = copy(
                own.at[spot], far_recv.at[spot], fs_s.at[spot], fs_r.at[spot],
                (2 * partner(outer, n_outer, step) + inner, mp),
            )
            each.start()
            far.append(each)
    last = n_outer - 1
    total = own[last] + near_recv[last]

    for each in peak_copies:
        each.wait_recv()
    peaks = jnp.maximum(peaks, jnp.max(peak_recv[...], axis=0))
    peak2_send[...] = peaks
    peak2_copies = []
    for step in range(1, n_mp):
        each = copy(
            peak2_send, peak2_recv.at[step - 1], pm_s.at[step - 1], pm_r.at[step - 1],
            (dp, lax.rem(mp + step, n_mp)),
        )
        each.start()
        peak2_copies.append(each)

    for spot in range(last):
        far[spot].wait_recv()
        total = total + far_recv[spot]
    q_moment = MOMENTUM * qm_ref[0] + total[:q_rows]
    k_moment = MOMENTUM * km_ref[0] + total[q_rows:]
    qm_out[0] = q_moment
    km_out[0] = k_moment

    grams[0] = gram(q_moment)
    grams[1] = gram(k_moment)
    swap = copy(grams.at[1 - core], gram_recv, g_s, g_r, (dp, other_core))
    swap.start()
    swap.wait_recv()
    whole = grams[core] + gram_recv[...]
    rows = []
    if n_group > 1:
        row_send[...] = whole
        for step in range(1, n_group):
            each = copy(
                row_send, row_recv.at[step - 1], y_s.at[step - 1], y_r.at[step - 1],
                (dp, 2 * lax.rem(group + step, n_group) + core),
            )
            each.start()
            rows.append(each)
        for step in range(1, n_group):
            rows[step - 1].wait_recv()
            whole = whole + row_recv[step - 1]
    z_send[...] = whole
    cross = copy(z_send, z_recv, z_s, z_r, (lax.rem(dp + heads, n_dp), mp))
    cross.start()
    cross.wait_recv()
    whole = whole + z_recv[...]

    eye = (
        lax.broadcasted_iota(jnp.int32, (width, width), 0)
        == lax.broadcasted_iota(jnp.int32, (width, width), 1)
    ).astype(F32)
    trace = jnp.sum(jnp.sum(whole * eye, axis=0, keepdims=True), axis=1, keepdims=True)
    scale = 1.0 / jnp.sqrt(trace + 1.0)
    current = whole * (scale * scale)
    mixed = None
    for step in range(ITERS):
        parts = split(current)
        square = mm3(parts, parts)
        poly = COEFF_A * eye + COEFF_B * current + COEFF_C * square
        pair = split(poly)
        mixed = poly * scale if mixed is None else mm3(split(mixed), pair)
        if step + 1 < ITERS:
            current = mm3(split(mm3(parts, pair)), pair)
    mix[core] = mixed
    swap2 = copy(mix.at[core], mix.at[core], m_s, m_r, (dp, other_core))
    swap2.start()

    for each in peak2_copies:
        each.wait_recv()
    peaks = jnp.maximum(peaks, jnp.max(peak2_recv[...], axis=0))
    mine = jnp.where(lane == lax.rem(dp, heads), peaks, LOWEST)
    peak = jnp.max(jnp.max(mine, axis=0, keepdims=True), axis=1, keepdims=True)
    shrink = jnp.sqrt(CLIP_LEVEL / jnp.maximum(peak, CLIP_LEVEL))
    keep = 1.0 - STEP_SIZE * DECAY
    q_full = q_rows * n_mp * 2
    k_full = k_rows * n_mp * 2
    q_parts = split(q_moment)
    k_parts = split(k_moment)
    swap2.wait_recv()
    q_ortho = mm3(q_parts, split(mix[0]))
    k_ortho = mm3(k_parts, split(mix[1]))
    qw_out[0] = (qw_ref[0] * keep - (STEP_SIZE * 0.2 * math.sqrt(q_full)) * q_ortho) * shrink
    kw_out[0] = (kw_ref[0] * keep - (STEP_SIZE * 0.2 * math.sqrt(k_full)) * k_ortho) * shrink
    for each in near + far + peak_copies + peak2_copies + [swap] + rows + [cross, swap2]:
        each.wait_send()


def local(
    q_latent, kv_latent, q_head_grad, k_head_grad, q_heads, k_heads,
    query_pick, key_pick, q_weight, k_weight, q_moment, k_moment,
):
    n_dp = lax.axis_size("dp")
    n_mp = lax.axis_size("mp")
    heads = n_dp // 2
    n_outer = n_dp // 2
    n_group = max(n_mp // 2, 2)
    rows = q_latent.shape[2] + kv_latent.shape[2]
    width = q_moment.shape[2]
    latent = jnp.concatenate([q_latent, kv_latent], axis=2).transpose(1, 2, 0)
    vmem = pltpu.VMEM
    dma = pltpu.SemaphoreType.DMA
    square = (width, width)
    tile = (8, width)
    return pl.pallas_call(
        functools.partial(kernel, n_dp, n_mp, heads),
        out_shape=[jax.ShapeDtypeStruct(a.shape, F32) for a in (q_weight, k_weight, q_moment, k_moment)],
        in_specs=[pl.BlockSpec(memory_space=vmem)] * 11,
        out_specs=[pl.BlockSpec(memory_space=vmem)] * 4,
        scratch_shapes=[
            vmem((n_outer, rows, width), F32),
            vmem((n_outer, rows, width), F32),
            vmem((n_outer, rows, width), F32),
            vmem((n_outer, rows, width), F32),
            vmem(tile, F32),
            vmem((n_dp - 1,) + tile, F32),
            vmem(tile, F32),
            vmem((n_mp - 1,) + tile, F32),
            vmem((2,) + square, F32),
            vmem(square, F32),
            vmem(square, F32),
            vmem((n_group - 1,) + square, F32),
            vmem(square, F32),
            vmem(square, F32),
            vmem((2,) + square, F32),
            dma((n_outer,)), dma((n_outer,)),
            dma((n_outer,)), dma((n_outer,)),
            dma((n_dp - 1,)), dma((n_dp - 1,)),
            dma((n_mp - 1,)), dma((n_mp - 1,)),
            dma, dma,
            dma((n_group - 1,)), dma((n_group - 1,)),
            dma, dma,
            dma, dma,
        ],
        compiler_params=pltpu.CompilerParams(
            collective_id=0, has_side_effects=True, vmem_limit_bytes=56 * 1024 * 1024
        ),
    )(
        latent, q_head_grad, k_head_grad, q_heads, k_heads,
        query_pick, key_pick, q_weight, k_weight, q_moment, k_moment,
    )


def solution(mesh):
    rows3 = P("dp", "mp", None)
    in_specs = (
        P("dp", None, "mp"), P("dp", None, "mp"), P("dp", None), P("dp", None),
        P("dp", "mp"), P("dp", "mp"), P("dp", None, "mp"), P("dp", None, "mp"),
        rows3, rows3, rows3, rows3,
    )
    return jax.shard_map(
        lambda *args: tuple(local(*args)),
        mesh=mesh, in_specs=in_specs, out_specs=(rows3,) * 4, check_vma=False,
    )
```

```python
import functools
import math

import jax
import jax.numpy as jnp
from jax import lax
from jax.experimental import pallas as pl
from jax.experimental.pallas import tpu as pltpu
from jax.sharding import PartitionSpec as P

ITERS = 5
MOMENTUM = 0.95
STEP_SIZE = 1.0
DECAY = 0.1
CLIP_LEVEL = 0.1
SCORE_SCALE = 1.0 / math.sqrt(192.0)
COEFF_A = 3.4445
COEFF_B = -4.775
COEFF_C = 2.0315
LOWEST = -1e30
MESH = pl.DeviceIdType.MESH
F32 = jnp.float32
BF16 = jnp.bfloat16


def split(value):
    high = value.astype(BF16)
    return high, (value - high.astype(F32)).astype(BF16)


def mm(a, b):
    return jnp.dot(a, b, preferred_element_type=F32)


def mm3(a, b):
    return mm(a[0], b[0]) + (mm(a[0], b[1]) + mm(a[1], b[0]))


def gram(rows):
    high, low = split(rows)
    high_t = high.T
    cross = mm(high_t, low)
    return mm(high_t, high) + (cross + cross.T)


def fold(matrix):
    width = matrix.shape[0]
    half = width // 2
    row = lax.broadcasted_iota(jnp.int32, (half, width), 0)
    lane = lax.broadcasted_iota(jnp.int32, (half, width), 1)
    lower = matrix[half:]
    body = jnp.where(lane >= row, matrix[:half], pltpu.roll(lower, half, 1))
    ends = jnp.sum(jnp.where(lane == row + half, lower, 0.0), axis=0, keepdims=True)
    return body, jnp.broadcast_to(ends, (8, width))


def unfold(message):
    width = message.shape[1]
    half = width // 2
    row = lax.broadcasted_iota(jnp.int32, (half, width), 0)
    lane = lax.broadcasted_iota(jnp.int32, (half, width), 1)
    body = message[:half]
    ends = jnp.broadcast_to(message[half : half + 1], (half, width))
    top = jnp.where(lane >= row, body, 0.0)
    strict = jnp.where((lane >= half) & (lane - half < row), pltpu.roll(body, half, 1), 0.0)
    one_side = jnp.concatenate([top, jnp.where(lane == row + half, ends, strict)], axis=0)
    full_row = lax.broadcasted_iota(jnp.int32, (width, width), 0)
    full_lane = lax.broadcasted_iota(jnp.int32, (width, width), 1)
    return one_side + jnp.where(full_row == full_lane, 0.0, one_side.T)


def column(row):
    count = row.shape[1]
    spread = jnp.broadcast_to(row, (count, count))
    same = lax.broadcasted_iota(jnp.int32, (count, count), 0) == lax.broadcasted_iota(
        jnp.int32, (count, count), 1
    )
    picked = jnp.where(same, spread, 0).astype(F32)
    return jnp.sum(picked, axis=1, keepdims=True).astype(jnp.int32)


def partner(index, count, step):
    if count & (count - 1):
        return lax.rem(index + step, count)
    result = 0
    bit = 1
    while bit < count:
        held = lax.rem(lax.div(index, bit), 2)
        result = result + bit * ((1 - held) if step & bit else held)
        bit *= 2
    return result


def kernel(
    n_dp, n_mp, heads,
    ql_in, kl_in, qg_in, kg_in, qh_in, kh_in, qp_in, kp_in, qw_in, kw_in, qm_in, km_in,
    qw_out, kw_out, qm_out, km_out, mix, shrink_out,
    ql_ref, kl_ref, qg_ref, kg_ref, qh_ref, kh_ref, qp_ref, kp_ref, qw_ref, kw_ref, qm_ref, km_ref, in_sems,
    near_send, near_recv, own, far_recv, peak_send, peak_recv, peak2_send, peak2_recv,
    grams, gram_recv, row_send, row_recv, z_send, z_recv,
    ns_s, ns_r, fs_s, fs_r, pk_s, pk_r, pm_s, pm_r, g_s, g_r, y_s, y_r, z_s, z_r, m_s, m_r,
):
    dp = lax.axis_index("dp")
    mp = lax.axis_index("mp")
    n_outer = n_dp // 2
    outer = lax.div(dp, 2)
    inner = lax.rem(dp, 2)
    core = lax.rem(mp, 2)
    group = lax.div(mp, 2)
    n_group = n_mp // 2
    q_rows = qm_ref.shape[1]
    k_rows = km_ref.shape[1]
    width = qm_ref.shape[2]
    tokens = qg_ref.shape[0]
    other_core = mp + 1 - 2 * core

    barrier = pltpu.get_barrier_semaphore()
    for step in range(1, n_dp):
        pl.semaphore_signal(
            barrier, inc=1, device_id=(lax.rem(dp + step, n_dp), mp), device_id_type=MESH
        )
    for step in range(1, n_mp):
        pl.semaphore_signal(
            barrier, inc=1, device_id=(dp, lax.rem(mp + step, n_mp)), device_id_type=MESH
        )

    loads = [
        pltpu.make_async_copy(src, dst, in_sems.at[i])
        for i, (src, dst) in enumerate((
            (ql_in, ql_ref), (kl_in, kl_ref), (qg_in, qg_ref), (kg_in, kg_ref),
            (qp_in, qp_ref), (kp_in, kp_ref), (qh_in, qh_ref), (kh_in, kh_ref),
            (qm_in, qm_ref), (km_in, km_ref), (qw_in, qw_ref), (kw_in, kw_ref),
        ))
    ]
    for each in loads:
        each.start()

    def copy(src, dst, send, recv, where):
        return pltpu.make_async_remote_copy(
            src_ref=src, dst_ref=dst, send_sem=send, recv_sem=recv,
            device_id=where, device_id_type=MESH,
        )

    def term(dst, where, to_outer, to_inner):
        slot = 2 * to_outer + to_inner
        half = lax.div(slot, heads)
        cols = pl.ds(pl.multiple_of(lax.rem(slot, heads) * width, width), width)
        dst[where, :q_rows, :] = mm(ql_ref[half], qg_ref[:, cols])
        dst[where, q_rows:, :] = mm(kl_ref[half], kg_ref[:, cols])

    for each in loads[:4]:
        each.wait()
    order = list(range(n_outer - 1, -1, -1))
    neighbour = (dp + 1 - 2 * inner, mp)
    near = []
    for spot, step in enumerate(order):
        term(near_send, spot, partner(outer, n_outer, step), 1 - inner)
        if spot == 0:
            pl.semaphore_wait(barrier, n_dp + n_mp - 2)
        each = copy(near_send.at[spot], near_recv.at[spot], ns_s.at[spot], ns_r.at[spot], neighbour)
        each.start()
        near.append(each)

    for each in loads[4:8]:
        each.wait()
    local_heads = qp_ref.shape[0]
    lane = lax.broadcasted_iota(jnp.int32, (8, width), 1)
    peaks = jnp.full((8, width), LOWEST, F32)
    ids = lax.broadcasted_iota(jnp.int32, (qp_ref.shape[2], tokens), 1)
    for head in range(local_heads):
        span = slice(head * width, (head + 1) * width)
        pick_q = (ids == column(qp_ref[head])).astype(F32).astype(BF16)
        pick_k = (ids == column(kp_ref[head])).astype(F32).astype(BF16)
        score = jnp.sum(
            mm(pick_q, qh_ref[:, span]) * mm(pick_k, kh_ref[:, span]), axis=1, keepdims=True
        )
        top = jnp.max(score * SCORE_SCALE, axis=0, keepdims=True)
        peaks = jnp.where(lane == mp * local_heads + head, top, peaks)
    peak_send[...] = peaks
    peak_copies = []
    for step in range(1, n_dp):
        each = copy(
            peak_send, peak_recv.at[step - 1], pk_s.at[step - 1], pk_r.at[step - 1],
            (lax.rem(dp + step, n_dp), mp),
        )
        each.start()
        peak_copies.append(each)

    for spot, step in enumerate(order):
        term(own, spot, partner(outer, n_outer, step), inner)
    far = []
    for spot, step in enumerate(order):
        near[spot].wait_recv()
        if step:
            own[spot] = own[spot] + near_recv[spot]
            each = copy(
                own.at[spot], far_recv.at[spot], fs_s.at[spot], fs_r.at[spot],
                (2 * partner(outer, n_outer, step) + inner, mp),
            )
            each.start()
            far.append(each)
    last = n_outer - 1
    total = own[last] + near_recv[last]

    for each in peak_copies:
        each.wait_recv()
    peaks = jnp.maximum(peaks, jnp.max(peak_recv[...], axis=0))
    peak2_send[...] = peaks
    peak2_copies = []
    for step in range(1, n_mp):
        each = copy(
            peak2_send, peak2_recv.at[step - 1], pm_s.at[step - 1], pm_r.at[step - 1],
            (dp, lax.rem(mp + step, n_mp)),
        )
        each.start()
        peak2_copies.append(each)

    for spot in range(last):
        far[spot].wait_recv()
        total = total + far_recv[spot]
    for each in loads[8:]:
        each.wait()
    q_moment = MOMENTUM * qm_ref[0] + total[:q_rows]
    k_moment = MOMENTUM * km_ref[0] + total[q_rows:]
    qm_out[0] = q_moment
    km_out[0] = k_moment

    top = width // 2
    for which, matrix in enumerate((gram(q_moment), gram(k_moment))):
        body, ends = fold(matrix)
        grams[which, :top, :] = body
        grams[which, top:, :] = ends
    swap = copy(grams.at[1 - core], gram_recv, g_s, g_r, (dp, other_core))
    swap.start()
    swap.wait_recv()
    whole = grams[core] + gram_recv[...]
    rows = []
    if n_group > 1:
        row_send[...] = whole
        for step in range(1, n_group):
            each = copy(
                row_send, row_recv.at[step - 1], y_s.at[step - 1], y_r.at[step - 1],
                (dp, 2 * lax.rem(group + step, n_group) + core),
            )
            each.start()
            rows.append(each)
        for step in range(1, n_group):
            rows[step - 1].wait_recv()
            whole = whole + row_recv[step - 1]
    z_send[...] = whole
    cross = copy(z_send, z_recv, z_s, z_r, (lax.rem(dp + heads, n_dp), mp))
    cross.start()
    cross.wait_recv()
    whole = unfold(whole + z_recv[...])

    eye = (
        lax.broadcasted_iota(jnp.int32, (width, width), 0)
        == lax.broadcasted_iota(jnp.int32, (width, width), 1)
    ).astype(F32)
    trace = jnp.sum(jnp.sum(whole * eye, axis=0, keepdims=True), axis=1, keepdims=True)
    scale = 1.0 / jnp.sqrt(trace + 1.0)
    current = whole * (scale * scale)
    mixed = None
    for step in range(ITERS):
        parts = split(current)
        square = mm3(parts, parts)
        poly = COEFF_A * eye + COEFF_B * current + COEFF_C * square
        pair = split(poly)
        mixed = poly * scale if mixed is None else mm3(split(mixed), pair)
        if step + 1 < ITERS:
            current = mm3(split(mm3(parts, pair)), pair)
    mix[core] = mixed
    swap2 = copy(mix.at[core], mix.at[core], m_s, m_r, (dp, other_core))
    swap2.start()

    for each in peak2_copies:
        each.wait_recv()
    peaks = jnp.maximum(peaks, jnp.max(peak2_recv[...], axis=0))
    mine = jnp.where(lane == lax.rem(dp, heads), peaks, LOWEST)
    peak = jnp.max(jnp.max(mine, axis=0, keepdims=True), axis=1, keepdims=True)
    shrink = jnp.sqrt(CLIP_LEVEL / jnp.maximum(peak, CLIP_LEVEL))
    keep = 1.0 - STEP_SIZE * DECAY
    shrink_out[...] = jnp.broadcast_to(shrink, shrink_out.shape)
    qw_out[0] = (qw_ref[0] * keep) * shrink
    kw_out[0] = (kw_ref[0] * keep) * shrink
    swap2.wait_recv()
    for each in near + far + peak_copies + peak2_copies + [swap] + rows + [cross, swap2]:
        each.wait_send()


def finish(n_mp, qw_ref, kw_ref, qm_ref, km_ref, mix_ref, shrink_ref, qw_out, kw_out, qm_out, km_out):
    groups = ((qw_ref, qm_ref, qw_out, qm_out), (kw_ref, km_ref, kw_out, km_out))
    for which, (weight, moment, weight_out, moment_out) in enumerate(groups):
        rows = moment[0]
        size = STEP_SIZE * 0.2 * math.sqrt(2 * n_mp * rows.shape[0])
        ortho = mm3(split(rows), split(mix_ref[which]))
        moment_out[0] = rows
        weight_out[0] = weight[0] - (size * ortho) * shrink_ref[0:1, :]


def local(
    q_latent, kv_latent, q_head_grad, k_head_grad, q_heads, k_heads,
    query_pick, key_pick, q_weight, k_weight, q_moment, k_moment,
):
    n_dp = lax.axis_size("dp")
    n_mp = lax.axis_size("mp")
    heads = n_dp // 2
    n_outer = n_dp // 2
    n_group = max(n_mp // 2, 2)
    rows = q_latent.shape[2] + kv_latent.shape[2]
    width = q_moment.shape[2]
    operands = (
        q_latent.transpose(1, 2, 0), kv_latent.transpose(1, 2, 0), q_head_grad, k_head_grad,
        q_heads, k_heads, query_pick.transpose(2, 0, 1), key_pick.transpose(2, 0, 1),
        q_weight, k_weight, q_moment, k_moment,
    )
    vmem = pltpu.VMEM
    dma = pltpu.SemaphoreType.DMA
    square = (width, width)
    folded = (width // 2 + 8, width)
    tile = (8, width)
    shapes = [a.shape for a in (q_weight, k_weight, q_moment, k_moment)]
    parts = pl.pallas_call(
        functools.partial(kernel, n_dp, n_mp, heads),
        out_shape=[vmem(shape, F32) for shape in shapes + [(2,) + square, tile]],
        in_specs=[pl.BlockSpec(memory_space=pl.ANY)] * 12,
        out_specs=[pl.BlockSpec(memory_space=vmem)] * 6,
        scratch_shapes=[vmem(a.shape, a.dtype) for a in operands] + [
            dma((12,)),
            vmem((n_outer, rows, width), F32),
            vmem((n_outer, rows, width), F32),
            vmem((n_outer, rows, width), F32),
            vmem((n_outer, rows, width), F32),
            vmem(tile, F32),
            vmem((n_dp - 1,) + tile, F32),
            vmem(tile, F32),
            vmem((n_mp - 1,) + tile, F32),
            vmem((2,) + folded, F32),
            vmem(folded, F32),
            vmem(folded, F32),
            vmem((n_group - 1,) + folded, F32),
            vmem(folded, F32),
            vmem(folded, F32),
            dma((n_outer,)), dma((n_outer,)),
            dma((n_outer,)), dma((n_outer,)),
            dma((n_dp - 1,)), dma((n_dp - 1,)),
            dma((n_mp - 1,)), dma((n_mp - 1,)),
            dma, dma,
            dma((n_group - 1,)), dma((n_group - 1,)),
            dma, dma,
            dma, dma,
        ],
        compiler_params=pltpu.CompilerParams(
            collective_id=0, has_side_effects=True, vmem_limit_bytes=56 * 1024 * 1024
        ),
    )(*operands)
    return pl.pallas_call(
        functools.partial(finish, n_mp),
        out_shape=[jax.ShapeDtypeStruct(shape, F32) for shape in shapes],
        in_specs=[pl.BlockSpec(memory_space=vmem)] * 6,
        out_specs=[pl.BlockSpec(memory_space=vmem)] * 4,
    )(*[pltpu.with_memory_space_constraint(part, vmem) for part in parts])


def solution(mesh):
    rows3 = P("dp", "mp", None)
    in_specs = (
        P("dp", None, "mp"), P("dp", None, "mp"), P("dp", None), P("dp", None),
        P("dp", "mp"), P("dp", "mp"), P("dp", None, "mp"), P("dp", None, "mp"),
        rows3, rows3, rows3, rows3,
    )
    return jax.shard_map(
        lambda *args: tuple(local(*args)),
        mesh=mesh, in_specs=in_specs, out_specs=(rows3,) * 4, check_vma=False,
    )
```

```python
import functools
import math

import jax
import jax.numpy as jnp
from jax import lax
from jax.experimental import pallas as pl
from jax.experimental.pallas import tpu as pltpu
from jax.sharding import PartitionSpec as P

ITERS = 5
MOMENTUM = 0.95
STEP_SIZE = 1.0
DECAY = 0.1
CLIP_LEVEL = 0.1
SCORE_SCALE = 1.0 / math.sqrt(192.0)
COEFF_A = 3.4445
COEFF_B = -4.775
COEFF_C = 2.0315
LOWEST = -1e30
MESH = pl.DeviceIdType.MESH
F32 = jnp.float32
BF16 = jnp.bfloat16


def split(value):
    high = value.astype(BF16)
    return high, (value - high.astype(F32)).astype(BF16)


def mm(a, b):
    return jnp.dot(a, b, preferred_element_type=F32)


def mm3(a, b):
    return mm(a[0], b[0]) + (mm(a[0], b[1]) + mm(a[1], b[0]))


def gram(rows):
    high, low = split(rows)
    high_t = high.T
    cross = mm(high_t, low)
    return mm(high_t, high) + (cross + cross.T)


def fold(matrix):
    width = matrix.shape[0]
    half = width // 2
    row = lax.broadcasted_iota(jnp.int32, (half, width), 0)
    lane = lax.broadcasted_iota(jnp.int32, (half, width), 1)
    lower = matrix[half:]
    body = jnp.where(lane >= row, matrix[:half], pltpu.roll(lower, half, 1))
    ends = jnp.sum(jnp.where(lane == row + half, lower, 0.0), axis=0, keepdims=True)
    return body, jnp.broadcast_to(ends, (8, width))


def unfold(message):
    width = message.shape[1]
    half = width // 2
    row = lax.broadcasted_iota(jnp.int32, (half, width), 0)
    lane = lax.broadcasted_iota(jnp.int32, (half, width), 1)
    body = message[:half]
    ends = jnp.broadcast_to(message[half : half + 1], (half, width))
    top = jnp.where(lane >= row, body, 0.0)
    strict = jnp.where((lane >= half) & (lane - half < row), pltpu.roll(body, half, 1), 0.0)
    one_side = jnp.concatenate([top, jnp.where(lane == row + half, ends, strict)], axis=0)
    full_row = lax.broadcasted_iota(jnp.int32, (width, width), 0)
    full_lane = lax.broadcasted_iota(jnp.int32, (width, width), 1)
    return one_side + jnp.where(full_row == full_lane, 0.0, one_side.T)


def column(row):
    count = row.shape[1]
    spread = jnp.broadcast_to(row, (count, count))
    same = lax.broadcasted_iota(jnp.int32, (count, count), 0) == lax.broadcasted_iota(
        jnp.int32, (count, count), 1
    )
    picked = jnp.where(same, spread, 0).astype(F32)
    return jnp.sum(picked, axis=1, keepdims=True).astype(jnp.int32)


def partner(index, count, step):
    if count & (count - 1):
        return lax.rem(index + step, count)
    result = 0
    bit = 1
    while bit < count:
        held = lax.rem(lax.div(index, bit), 2)
        result = result + bit * ((1 - held) if step & bit else held)
        bit *= 2
    return result


def kernel(
    n_dp, n_mp, heads,
    ql_in, kl_in, qg_in, kg_in, qh_in, kh_in, qp_in, kp_in, qw_in, kw_in, qm_in, km_in,
    qw_out, kw_out, qm_out, km_out, mix, shrink_out,
    ql_ref, kl_ref, qg_ref, kg_ref, qh_ref, kh_ref, qp_ref, kp_ref, qw_ref, kw_ref, qm_ref, km_ref, in_sems,
    near_send, near_recv, own, far_recv, peak_send, peak_recv, peak2_send, peak2_recv,
    grams, gram_recv, row_send, row_recv, z_send, z_recv,
    ns_s, ns_r, fs_s, fs_r, pk_s, pk_r, pm_s, pm_r, g_s, g_r, y_s, y_r, z_s, z_r, m_s, m_r,
):
    dp = lax.axis_index("dp")
    mp = lax.axis_index("mp")
    n_outer = n_dp // 2
    outer = lax.div(dp, 2)
    inner = lax.rem(dp, 2)
    core = lax.rem(mp, 2)
    group = lax.div(mp, 2)
    n_group = n_mp // 2
    q_rows = qm_ref.shape[1]
    k_rows = km_ref.shape[1]
    width = qm_ref.shape[2]
    tokens = qg_ref.shape[0]
    other_core = mp + 1 - 2 * core

    barrier = pltpu.get_barrier_semaphore()
    for step in range(1, n_dp):
        pl.semaphore_signal(
            barrier, inc=1, device_id=(lax.rem(dp + step, n_dp), mp), device_id_type=MESH
        )
    for step in range(1, n_mp):
        pl.semaphore_signal(
            barrier, inc=1, device_id=(dp, lax.rem(mp + step, n_mp)), device_id_type=MESH
        )

    loads = [
        pltpu.make_async_copy(src, dst, in_sems.at[i])
        for i, (src, dst) in enumerate((
            (ql_in, ql_ref), (kl_in, kl_ref), (qg_in, qg_ref), (kg_in, kg_ref),
            (qp_in, qp_ref), (kp_in, kp_ref), (qh_in, qh_ref), (kh_in, kh_ref),
            (qm_in, qm_ref), (km_in, km_ref), (qw_in, qw_ref), (kw_in, kw_ref),
        ))
    ]
    for each in loads:
        each.start()

    def copy(src, dst, send, recv, where):
        return pltpu.make_async_remote_copy(
            src_ref=src, dst_ref=dst, send_sem=send, recv_sem=recv,
            device_id=where, device_id_type=MESH,
        )

    def term(dst, where, to_outer, to_inner):
        slot = 2 * to_outer + to_inner
        half = lax.div(slot, heads)
        cols = pl.ds(pl.multiple_of(lax.rem(slot, heads) * width, width), width)
        dst[where, :q_rows, :] = mm(ql_ref[half], qg_ref[:, cols])
        dst[where, q_rows:, :] = mm(kl_ref[half], kg_ref[:, cols])

    for each in loads[:4]:
        each.wait()
    order = list(range(n_outer - 1, -1, -1))
    neighbour = (dp + 1 - 2 * inner, mp)
    near = []
    for spot, step in enumerate(order):
        term(near_send, spot, partner(outer, n_outer, step), 1 - inner)
        if spot == 0:
            pl.semaphore_wait(barrier, n_dp + n_mp - 2)
        each = copy(near_send.at[spot], near_recv.at[spot], ns_s.at[spot], ns_r.at[spot], neighbour)
        each.start()
        near.append(each)

    for each in loads[4:8]:
        each.wait()
    local_heads = qp_ref.shape[0]
    lane = lax.broadcasted_iota(jnp.int32, (8, width), 1)
    peaks = jnp.full((8, width), LOWEST, F32)
    ids = lax.broadcasted_iota(jnp.int32, (qp_ref.shape[2], tokens), 1)
    for head in range(local_heads):
        span = slice(head * width, (head + 1) * width)
        pick_q = (ids == column(qp_ref[head])).astype(F32).astype(BF16)
        pick_k = (ids == column(kp_ref[head])).astype(F32).astype(BF16)
        score = jnp.sum(
            mm(pick_q, qh_ref[:, span]) * mm(pick_k, kh_ref[:, span]), axis=1, keepdims=True
        )
        top = jnp.max(score * SCORE_SCALE, axis=0, keepdims=True)
        peaks = jnp.where(lane == mp * local_heads + head, top, peaks)
    peak_send[...] = peaks
    peak_copies = []
    for step in range(1, n_dp):
        each = copy(
            peak_send, peak_recv.at[step - 1], pk_s.at[step - 1], pk_r.at[step - 1],
            (lax.rem(dp + step, n_dp), mp),
        )
        each.start()
        peak_copies.append(each)

    for spot, step in enumerate(order):
        term(own, spot, partner(outer, n_outer, step), inner)
    last = n_outer - 1
    relayed = n_outer == 4
    inside = lax.rem(lax.div(outer, 2) + lax.rem(outer, 2), 2)
    far = []
    for spot, step in enumerate(order):
        near[spot].wait_recv()
        if not step:
            continue
        own[spot] = own[spot] + near_recv[spot]
        where = spot
        target = partner(outer, n_outer, step)
        if relayed and spot == 0:
            where = last * (1 - inside)
            aside = partner(outer, n_outer, 1)
            target = aside + inside * (target - aside)
        if relayed and spot == 1:

            @pl.when(inside == 1)
            def _():
                copy(
                    own.at[0], far_recv.at[last], fs_s.at[0], fs_r.at[last], (dp, mp)
                ).wait_recv()
                own[1] = own[1] + far_recv[last]

        each = copy(
            own.at[spot], far_recv.at[where], fs_s.at[spot], fs_r.at[where],
            (2 * target + inner, mp),
        )
        each.start()
        far.append(each)
    own[last] = own[last] + near_recv[last]

    for each in peak_copies:
        each.wait_recv()
    peaks = jnp.maximum(peaks, jnp.max(peak_recv[...], axis=0))
    peak2_send[...] = peaks
    peak2_copies = []
    for step in range(1, n_mp):
        each = copy(
            peak2_send, peak2_recv.at[step - 1], pm_s.at[step - 1], pm_r.at[step - 1],
            (dp, lax.rem(mp + step, n_mp)),
        )
        each.start()
        peak2_copies.append(each)

    if relayed:

        @pl.when(inside == 1)
        def _():
            copy(own.at[0], far_recv.at[0], fs_s.at[0], fs_r.at[0], (dp, mp)).wait_recv()
            own[last] = own[last] + far_recv[0]

    total = own[last]
    for spot in range(1 if relayed else 0, last):
        far[spot].wait_recv()
        total = total + far_recv[spot]
    for each in loads[8:]:
        each.wait()
    q_moment = MOMENTUM * qm_ref[0] + total[:q_rows]
    k_moment = MOMENTUM * km_ref[0] + total[q_rows:]
    qm_out[0] = q_moment
    km_out[0] = k_moment

    top = width // 2
    for which, matrix in enumerate((gram(q_moment), gram(k_moment))):
        body, ends = fold(matrix)
        grams[which, :top, :] = body
        grams[which, top:, :] = ends
    swap = copy(grams.at[1 - core], gram_recv, g_s, g_r, (dp, other_core))
    swap.start()
    swap.wait_recv()
    whole = grams[core] + gram_recv[...]
    rows = []
    if n_group > 1:
        row_send[...] = whole
        for step in range(1, n_group):
            each = copy(
                row_send, row_recv.at[step - 1], y_s.at[step - 1], y_r.at[step - 1],
                (dp, 2 * lax.rem(group + step, n_group) + core),
            )
            each.start()
            rows.append(each)
        for step in range(1, n_group):
            rows[step - 1].wait_recv()
            whole = whole + row_recv[step - 1]
    z_send[...] = whole
    cross = copy(z_send, z_recv, z_s, z_r, (lax.rem(dp + heads, n_dp), mp))
    cross.start()
    cross.wait_recv()
    whole = unfold(whole + z_recv[...])

    eye = (
        lax.broadcasted_iota(jnp.int32, (width, width), 0)
        == lax.broadcasted_iota(jnp.int32, (width, width), 1)
    ).astype(F32)
    trace = jnp.sum(jnp.sum(whole * eye, axis=0, keepdims=True), axis=1, keepdims=True)
    scale = 1.0 / jnp.sqrt(trace + 1.0)
    current = whole * (scale * scale)
    mixed = None
    for step in range(ITERS):
        parts = split(current)
        square = mm3(parts, parts)
        poly = COEFF_A * eye + COEFF_B * current + COEFF_C * square
        pair = split(poly)
        mixed = poly * scale if mixed is None else mm3(split(mixed), pair)
        if step + 1 < ITERS:
            current = mm3(split(mm3(parts, pair)), pair)
    mix[core] = mixed
    swap2 = copy(mix.at[core], mix.at[core], m_s, m_r, (dp, other_core))
    swap2.start()

    for each in peak2_copies:
        each.wait_recv()
    peaks = jnp.maximum(peaks, jnp.max(peak2_recv[...], axis=0))
    mine = jnp.where(lane == lax.rem(dp, heads), peaks, LOWEST)
    peak = jnp.max(jnp.max(mine, axis=0, keepdims=True), axis=1, keepdims=True)
    shrink = jnp.sqrt(CLIP_LEVEL / jnp.maximum(peak, CLIP_LEVEL))
    keep = 1.0 - STEP_SIZE * DECAY
    shrink_out[...] = jnp.broadcast_to(shrink, shrink_out.shape)
    qw_out[0] = (qw_ref[0] * keep) * shrink
    kw_out[0] = (kw_ref[0] * keep) * shrink
    swap2.wait_recv()
    for each in near + far + peak_copies + peak2_copies + [swap] + rows + [cross, swap2]:
        each.wait_send()


def finish(n_mp, qw_ref, kw_ref, qm_ref, km_ref, mix_ref, shrink_ref, qw_out, kw_out, qm_out, km_out):
    groups = ((qw_ref, qm_ref, qw_out, qm_out), (kw_ref, km_ref, kw_out, km_out))
    for which, (weight, moment, weight_out, moment_out) in enumerate(groups):
        rows = moment[0]
        size = STEP_SIZE * 0.2 * math.sqrt(2 * n_mp * rows.shape[0])
        ortho = mm3(split(rows), split(mix_ref[which]))
        moment_out[0] = rows
        weight_out[0] = weight[0] - (size * ortho) * shrink_ref[0:1, :]


def local(
    q_latent, kv_latent, q_head_grad, k_head_grad, q_heads, k_heads,
    query_pick, key_pick, q_weight, k_weight, q_moment, k_moment,
):
    n_dp = lax.axis_size("dp")
    n_mp = lax.axis_size("mp")
    heads = n_dp // 2
    n_outer = n_dp // 2
    n_group = max(n_mp // 2, 2)
    rows = q_latent.shape[2] + kv_latent.shape[2]
    width = q_moment.shape[2]
    operands = (
        q_latent.transpose(1, 2, 0), kv_latent.transpose(1, 2, 0), q_head_grad, k_head_grad,
        q_heads, k_heads, query_pick.transpose(2, 0, 1), key_pick.transpose(2, 0, 1),
        q_weight, k_weight, q_moment, k_moment,
    )
    vmem = pltpu.VMEM
    dma = pltpu.SemaphoreType.DMA
    square = (width, width)
    folded = (width // 2 + 8, width)
    tile = (8, width)
    shapes = [a.shape for a in (q_weight, k_weight, q_moment, k_moment)]
    parts = pl.pallas_call(
        functools.partial(kernel, n_dp, n_mp, heads),
        out_shape=[vmem(shape, F32) for shape in shapes + [(2,) + square, tile]],
        in_specs=[pl.BlockSpec(memory_space=pl.ANY)] * 12,
        out_specs=[pl.BlockSpec(memory_space=vmem)] * 6,
        scratch_shapes=[vmem(a.shape, a.dtype) for a in operands] + [
            dma((12,)),
            vmem((n_outer, rows, width), F32),
            vmem((n_outer, rows, width), F32),
            vmem((n_outer, rows, width), F32),
            vmem((n_outer, rows, width), F32),
            vmem(tile, F32),
            vmem((n_dp - 1,) + tile, F32),
            vmem(tile, F32),
            vmem((n_mp - 1,) + tile, F32),
            vmem((2,) + folded, F32),
            vmem(folded, F32),
            vmem(folded, F32),
            vmem((n_group - 1,) + folded, F32),
            vmem(folded, F32),
            vmem(folded, F32),
            dma((n_outer,)), dma((n_outer,)),
            dma((n_outer,)), dma((n_outer,)),
            dma((n_dp - 1,)), dma((n_dp - 1,)),
            dma((n_mp - 1,)), dma((n_mp - 1,)),
            dma, dma,
            dma((n_group - 1,)), dma((n_group - 1,)),
            dma, dma,
            dma, dma,
        ],
        compiler_params=pltpu.CompilerParams(
            collective_id=0, has_side_effects=True, vmem_limit_bytes=56 * 1024 * 1024
        ),
    )(*operands)
    return pl.pallas_call(
        functools.partial(finish, n_mp),
        out_shape=[jax.ShapeDtypeStruct(shape, F32) for shape in shapes],
        in_specs=[pl.BlockSpec(memory_space=vmem)] * 6,
        out_specs=[pl.BlockSpec(memory_space=vmem)] * 4,
    )(*[pltpu.with_memory_space_constraint(part, vmem) for part in parts])


def solution(mesh):
    rows3 = P("dp", "mp", None)
    in_specs = (
        P("dp", None, "mp"), P("dp", None, "mp"), P("dp", None), P("dp", None),
        P("dp", "mp"), P("dp", "mp"), P("dp", None, "mp"), P("dp", None, "mp"),
        rows3, rows3, rows3, rows3,
    )
    return jax.shard_map(
        lambda *args: tuple(local(*args)),
        mesh=mesh, in_specs=in_specs, out_specs=(rows3,) * 4, check_vma=False,
    )
```

```python
import functools
import math

import jax
import jax.numpy as jnp
from jax import lax
from jax.experimental import pallas as pl
from jax.experimental.pallas import tpu as pltpu
from jax.sharding import PartitionSpec as P

ITERS = 5
MOMENTUM = 0.95
STEP_SIZE = 1.0
DECAY = 0.1
CLIP_LEVEL = 0.1
SCORE_SCALE = 1.0 / math.sqrt(192.0)
COEFF_A = 3.4445
COEFF_B = -4.775
COEFF_C = 2.0315
LOWEST = -1e30
MESH = pl.DeviceIdType.MESH
F32 = jnp.float32
BF16 = jnp.bfloat16


def split(value):
    high = value.astype(BF16)
    return high, (value - high.astype(F32)).astype(BF16)


def mm(a, b):
    return jnp.dot(a, b, preferred_element_type=F32)


def mm3(a, b):
    return mm(a[0], b[0]) + (mm(a[0], b[1]) + mm(a[1], b[0]))


def gram(rows):
    high, low = split(rows)
    high_t = high.T
    cross = mm(high_t, low)
    return mm(high_t, high) + (cross + cross.T)


def fold(matrix):
    width = matrix.shape[0]
    half = width // 2
    row = lax.broadcasted_iota(jnp.int32, (half, width), 0)
    lane = lax.broadcasted_iota(jnp.int32, (half, width), 1)
    lower = matrix[half:]
    body = jnp.where(lane >= row, matrix[:half], pltpu.roll(lower, half, 1))
    ends = jnp.sum(jnp.where(lane == row + half, lower, 0.0), axis=0, keepdims=True)
    return body, jnp.broadcast_to(ends, (8, width))


def unfold(message):
    width = message.shape[1]
    half = width // 2
    row = lax.broadcasted_iota(jnp.int32, (half, width), 0)
    lane = lax.broadcasted_iota(jnp.int32, (half, width), 1)
    body = message[:half]
    ends = jnp.broadcast_to(message[half : half + 1], (half, width))
    top = jnp.where(lane >= row, body, 0.0)
    strict = jnp.where((lane >= half) & (lane - half < row), pltpu.roll(body, half, 1), 0.0)
    one_side = jnp.concatenate([top, jnp.where(lane == row + half, ends, strict)], axis=0)
    full_row = lax.broadcasted_iota(jnp.int32, (width, width), 0)
    full_lane = lax.broadcasted_iota(jnp.int32, (width, width), 1)
    return one_side + jnp.where(full_row == full_lane, 0.0, one_side.T)


def column(row):
    count = row.shape[1]
    spread = jnp.broadcast_to(row, (count, count))
    same = lax.broadcasted_iota(jnp.int32, (count, count), 0) == lax.broadcasted_iota(
        jnp.int32, (count, count), 1
    )
    picked = jnp.where(same, spread, 0).astype(F32)
    return jnp.sum(picked, axis=1, keepdims=True).astype(jnp.int32)


def partner(index, count, step):
    if count & (count - 1):
        return lax.rem(index + step, count)
    result = 0
    bit = 1
    while bit < count:
        held = lax.rem(lax.div(index, bit), 2)
        result = result + bit * ((1 - held) if step & bit else held)
        bit *= 2
    return result


def kernel(
    n_dp, n_mp, heads,
    ql_in, kl_in, qg_in, kg_in, qh_in, kh_in, qp_in, kp_in, qw_in, kw_in, qm_in, km_in,
    qw_out, kw_out, qm_out, km_out, mix, shrink_out,
    ql_ref, kl_ref, qg_ref, kg_ref, qh_ref, kh_ref, qp_ref, kp_ref, qw_ref, kw_ref, qm_ref, km_ref, in_sems,
    near_send, near_recv, own, far_recv, peak_send, peak_recv, peak2_send, peak2_recv,
    grams, gram_recv, row_send, row_recv,
    ns_s, ns_r, fs_s, fs_r, pk_s, pk_r, pm_s, pm_r, g_s, g_r, y_s, y_r, m_s, m_r,
):
    dp = lax.axis_index("dp")
    mp = lax.axis_index("mp")
    n_outer = n_dp // 2
    outer = lax.div(dp, 2)
    inner = lax.rem(dp, 2)
    core = lax.rem(mp, 2)
    group = lax.div(mp, 2)
    n_group = n_mp // 2
    q_rows = qm_ref.shape[1]
    k_rows = km_ref.shape[1]
    width = qm_ref.shape[2]
    tokens = qg_ref.shape[0]
    other_core = mp + 1 - 2 * core

    barrier = pltpu.get_barrier_semaphore()
    for step in range(1, n_dp):
        pl.semaphore_signal(
            barrier, inc=1, device_id=(lax.rem(dp + step, n_dp), mp), device_id_type=MESH
        )
    def owner(step):
        across = lax.rem(dp + (step // n_group) * heads, n_dp)
        return across, 2 * lax.rem(group + step, n_group) + core

    for step in range(n_group + 1, 2 * n_group):
        pl.semaphore_signal(barrier, inc=1, device_id=owner(step), device_id_type=MESH)
    for step in range(1, n_mp):
        pl.semaphore_signal(
            barrier, inc=1, device_id=(dp, lax.rem(mp + step, n_mp)), device_id_type=MESH
        )

    loads = [
        pltpu.make_async_copy(src, dst, in_sems.at[i])
        for i, (src, dst) in enumerate((
            (ql_in, ql_ref), (kl_in, kl_ref), (qg_in, qg_ref), (kg_in, kg_ref),
            (qp_in, qp_ref), (kp_in, kp_ref), (qh_in, qh_ref), (kh_in, kh_ref),
            (qm_in, qm_ref), (km_in, km_ref), (qw_in, qw_ref), (kw_in, kw_ref),
        ))
    ]
    for each in loads:
        each.start()

    def copy(src, dst, send, recv, where):
        return pltpu.make_async_remote_copy(
            src_ref=src, dst_ref=dst, send_sem=send, recv_sem=recv,
            device_id=where, device_id_type=MESH,
        )

    def term(dst, where, to_outer, to_inner):
        slot = 2 * to_outer + to_inner
        half = lax.div(slot, heads)
        cols = pl.ds(pl.multiple_of(lax.rem(slot, heads) * width, width), width)
        dst[where, :q_rows, :] = mm(ql_ref[half], qg_ref[:, cols])
        dst[where, q_rows:, :] = mm(kl_ref[half], kg_ref[:, cols])

    for each in loads[:4]:
        each.wait()
    order = list(range(n_outer - 1, -1, -1))
    neighbour = (dp + 1 - 2 * inner, mp)
    near = []
    for spot, step in enumerate(order):
        term(near_send, spot, partner(outer, n_outer, step), 1 - inner)
        if spot == 0:
            pl.semaphore_wait(barrier, n_dp + n_mp + n_group - 3)
        each = copy(near_send.at[spot], near_recv.at[spot], ns_s.at[spot], ns_r.at[spot], neighbour)
        each.start()
        near.append(each)

    for each in loads[4:8]:
        each.wait()
    local_heads = qp_ref.shape[0]
    lane = lax.broadcasted_iota(jnp.int32, (8, width), 1)
    peaks = jnp.full((8, width), LOWEST, F32)
    ids = lax.broadcasted_iota(jnp.int32, (qp_ref.shape[2], tokens), 1)
    for head in range(local_heads):
        span = slice(head * width, (head + 1) * width)
        pick_q = (ids == column(qp_ref[head])).astype(F32).astype(BF16)
        pick_k = (ids == column(kp_ref[head])).astype(F32).astype(BF16)
        score = jnp.sum(
            mm(pick_q, qh_ref[:, span]) * mm(pick_k, kh_ref[:, span]), axis=1, keepdims=True
        )
        top = jnp.max(score * SCORE_SCALE, axis=0, keepdims=True)
        peaks = jnp.where(lane == mp * local_heads + head, top, peaks)
    peak_send[...] = peaks
    peak_copies = []
    for step in range(1, n_dp):
        each = copy(
            peak_send, peak_recv.at[step - 1], pk_s.at[step - 1], pk_r.at[step - 1],
            (lax.rem(dp + step, n_dp), mp),
        )
        each.start()
        peak_copies.append(each)

    for spot, step in enumerate(order):
        term(own, spot, partner(outer, n_outer, step), inner)
    last = n_outer - 1
    relayed = n_outer == 4
    inside = lax.rem(lax.div(outer, 2) + lax.rem(outer, 2), 2)
    far = []
    for spot, step in enumerate(order):
        near[spot].wait_recv()
        if not step:
            continue
        own[spot] = own[spot] + near_recv[spot]
        where = spot
        target = partner(outer, n_outer, step)
        if relayed and spot == 0:
            where = last * (1 - inside)
            aside = partner(outer, n_outer, 1)
            target = aside + inside * (target - aside)
        if relayed and spot == 1:

            @pl.when(inside == 1)
            def _():
                copy(
                    own.at[0], far_recv.at[last], fs_s.at[0], fs_r.at[last], (dp, mp)
                ).wait_recv()
                own[1] = own[1] + far_recv[last]

        each = copy(
            own.at[spot], far_recv.at[where], fs_s.at[spot], fs_r.at[where],
            (2 * target + inner, mp),
        )
        each.start()
        far.append(each)
    own[last] = own[last] + near_recv[last]

    for each in peak_copies:
        each.wait_recv()
    peaks = jnp.maximum(peaks, jnp.max(peak_recv[...], axis=0))
    peak2_send[...] = peaks
    peak2_copies = []
    for step in range(1, n_mp):
        each = copy(
            peak2_send, peak2_recv.at[step - 1], pm_s.at[step - 1], pm_r.at[step - 1],
            (dp, lax.rem(mp + step, n_mp)),
        )
        each.start()
        peak2_copies.append(each)

    if relayed:

        @pl.when(inside == 1)
        def _():
            copy(own.at[0], far_recv.at[0], fs_s.at[0], fs_r.at[0], (dp, mp)).wait_recv()
            own[last] = own[last] + far_recv[0]

    total = own[last]
    for spot in range(1 if relayed else 0, last):
        far[spot].wait_recv()
        total = total + far_recv[spot]
    for each in loads[8:]:
        each.wait()
    q_moment = MOMENTUM * qm_ref[0] + total[:q_rows]
    k_moment = MOMENTUM * km_ref[0] + total[q_rows:]
    qm_out[0] = q_moment
    km_out[0] = k_moment

    top = width // 2
    for which, matrix in enumerate((gram(q_moment), gram(k_moment))):
        body, ends = fold(matrix)
        grams[which, :top, :] = body
        grams[which, top:, :] = ends
    swap = copy(grams.at[1 - core], gram_recv, g_s, g_r, (dp, other_core))
    swap.start()
    swap.wait_recv()
    whole = grams[core] + gram_recv[...]
    row_send[...] = whole
    rows = []
    for step in range(1, 2 * n_group):
        each = copy(
            row_send, row_recv.at[step - 1], y_s.at[step - 1], y_r.at[step - 1], owner(step)
        )
        each.start()
        rows.append(each)
    for each in rows:
        each.wait_recv()
    whole = unfold(whole + jnp.sum(row_recv[...], axis=0))

    eye = (
        lax.broadcasted_iota(jnp.int32, (width, width), 0)
        == lax.broadcasted_iota(jnp.int32, (width, width), 1)
    ).astype(F32)
    trace = jnp.sum(jnp.sum(whole * eye, axis=0, keepdims=True), axis=1, keepdims=True)
    scale = 1.0 / jnp.sqrt(trace + 1.0)
    current = whole * (scale * scale)
    mixed = None
    for step in range(ITERS):
        parts = split(current)
        square = mm3(parts, parts)
        poly = COEFF_A * eye + COEFF_B * current + COEFF_C * square
        pair = split(poly)
        mixed = poly * scale if mixed is None else mm3(split(mixed), pair)
        if step + 1 < ITERS:
            current = mm3(split(mm3(parts, pair)), pair)
    mix[core] = mixed
    swap2 = copy(mix.at[core], mix.at[core], m_s, m_r, (dp, other_core))
    swap2.start()

    for each in peak2_copies:
        each.wait_recv()
    peaks = jnp.maximum(peaks, jnp.max(peak2_recv[...], axis=0))
    mine = jnp.where(lane == lax.rem(dp, heads), peaks, LOWEST)
    peak = jnp.max(jnp.max(mine, axis=0, keepdims=True), axis=1, keepdims=True)
    shrink = jnp.sqrt(CLIP_LEVEL / jnp.maximum(peak, CLIP_LEVEL))
    keep = 1.0 - STEP_SIZE * DECAY
    shrink_out[...] = jnp.broadcast_to(shrink, shrink_out.shape)
    qw_out[0] = (qw_ref[0] * keep) * shrink
    kw_out[0] = (kw_ref[0] * keep) * shrink
    swap2.wait_recv()
    for each in near + far + peak_copies + peak2_copies + [swap] + rows + [swap2]:
        each.wait_send()


def finish(n_mp, qw_ref, kw_ref, qm_ref, km_ref, mix_ref, shrink_ref, qw_out, kw_out, qm_out, km_out):
    groups = ((qw_ref, qm_ref, qw_out, qm_out), (kw_ref, km_ref, kw_out, km_out))
    for which, (weight, moment, weight_out, moment_out) in enumerate(groups):
        rows = moment[0]
        size = STEP_SIZE * 0.2 * math.sqrt(2 * n_mp * rows.shape[0])
        ortho = mm3(split(rows), split(mix_ref[which]))
        moment_out[0] = rows
        weight_out[0] = weight[0] - (size * ortho) * shrink_ref[0:1, :]


def local(
    q_latent, kv_latent, q_head_grad, k_head_grad, q_heads, k_heads,
    query_pick, key_pick, q_weight, k_weight, q_moment, k_moment,
):
    n_dp = lax.axis_size("dp")
    n_mp = lax.axis_size("mp")
    heads = n_dp // 2
    n_outer = n_dp // 2
    n_group = n_mp // 2
    rows = q_latent.shape[2] + kv_latent.shape[2]
    width = q_moment.shape[2]
    operands = (
        q_latent.transpose(1, 2, 0), kv_latent.transpose(1, 2, 0), q_head_grad, k_head_grad,
        q_heads, k_heads, query_pick.transpose(2, 0, 1), key_pick.transpose(2, 0, 1),
        q_weight, k_weight, q_moment, k_moment,
    )
    vmem = pltpu.VMEM
    dma = pltpu.SemaphoreType.DMA
    square = (width, width)
    folded = (width // 2 + 8, width)
    tile = (8, width)
    shapes = [a.shape for a in (q_weight, k_weight, q_moment, k_moment)]
    parts = pl.pallas_call(
        functools.partial(kernel, n_dp, n_mp, heads),
        out_shape=[vmem(shape, F32) for shape in shapes + [(2,) + square, tile]],
        in_specs=[pl.BlockSpec(memory_space=pl.ANY)] * 12,
        out_specs=[pl.BlockSpec(memory_space=vmem)] * 6,
        scratch_shapes=[vmem(a.shape, a.dtype) for a in operands] + [
            dma((12,)),
            vmem((n_outer, rows, width), F32),
            vmem((n_outer, rows, width), F32),
            vmem((n_outer, rows, width), F32),
            vmem((n_outer, rows, width), F32),
            vmem(tile, F32),
            vmem((n_dp - 1,) + tile, F32),
            vmem(tile, F32),
            vmem((n_mp - 1,) + tile, F32),
            vmem((2,) + folded, F32),
            vmem(folded, F32),
            vmem(folded, F32),
            vmem((2 * n_group - 1,) + folded, F32),
            dma((n_outer,)), dma((n_outer,)),
            dma((n_outer,)), dma((n_outer,)),
            dma((n_dp - 1,)), dma((n_dp - 1,)),
            dma((n_mp - 1,)), dma((n_mp - 1,)),
            dma, dma,
            dma((2 * n_group - 1,)), dma((2 * n_group - 1,)),
            dma, dma,
        ],
        compiler_params=pltpu.CompilerParams(
            collective_id=0, has_side_effects=True, vmem_limit_bytes=56 * 1024 * 1024
        ),
    )(*operands)
    return pl.pallas_call(
        functools.partial(finish, n_mp),
        out_shape=[jax.ShapeDtypeStruct(shape, F32) for shape in shapes],
        in_specs=[pl.BlockSpec(memory_space=vmem)] * 6,
        out_specs=[pl.BlockSpec(memory_space=vmem)] * 4,
    )(*[pltpu.with_memory_space_constraint(part, vmem) for part in parts])


def solution(mesh):
    rows3 = P("dp", "mp", None)
    in_specs = (
        P("dp", None, "mp"), P("dp", None, "mp"), P("dp", None), P("dp", None),
        P("dp", "mp"), P("dp", "mp"), P("dp", None, "mp"), P("dp", None, "mp"),
        rows3, rows3, rows3, rows3,
    )
    return jax.shard_map(
        lambda *args: tuple(local(*args)),
        mesh=mesh, in_specs=in_specs, out_specs=(rows3,) * 4, check_vma=False,
    )
```

```python
import functools
import math

import jax
import jax.numpy as jnp
from jax import lax
from jax.experimental import pallas as pl
from jax.experimental.pallas import tpu as pltpu
from jax.sharding import PartitionSpec as P

ITERS = 5
MOMENTUM = 0.95
STEP_SIZE = 1.0
DECAY = 0.1
CLIP_LEVEL = 0.1
SCORE_SCALE = 1.0 / math.sqrt(192.0)
COEFF_A = 3.4445
COEFF_B = -4.775
COEFF_C = 2.0315
LOWEST = -1e30
MESH = pl.DeviceIdType.MESH
F32 = jnp.float32
BF16 = jnp.bfloat16


def split(value):
    high = value.astype(BF16)
    return high, (value - high.astype(F32)).astype(BF16)


def mm(a, b):
    return jnp.dot(a, b, preferred_element_type=F32)


def mm3(a, b):
    both = mm(a[0], jnp.concatenate([b[0], b[1]], axis=1))
    width = b[0].shape[1]
    return both[:, :width] + (both[:, width:] + mm(a[1], b[0]))


def gram(rows):
    high, low = split(rows)
    high_t = high.T
    cross = mm(high_t, low)
    return mm(high_t, high) + (cross + cross.T)


def fold(matrix):
    width = matrix.shape[0]
    half = width // 2
    row = lax.broadcasted_iota(jnp.int32, (half, width), 0)
    lane = lax.broadcasted_iota(jnp.int32, (half, width), 1)
    lower = matrix[half:]
    body = jnp.where(lane >= row, matrix[:half], pltpu.roll(lower, half, 1))
    ends = jnp.sum(jnp.where(lane == row + half, lower, 0.0), axis=0, keepdims=True)
    return body, jnp.broadcast_to(ends, (8, width))


def unfold(message):
    width = message.shape[1]
    half = width // 2
    row = lax.broadcasted_iota(jnp.int32, (half, width), 0)
    lane = lax.broadcasted_iota(jnp.int32, (half, width), 1)
    body = message[:half]
    ends = jnp.broadcast_to(message[half : half + 1], (half, width))
    top = jnp.where(lane >= row, body, 0.0)
    strict = jnp.where((lane >= half) & (lane - half < row), pltpu.roll(body, half, 1), 0.0)
    one_side = jnp.concatenate([top, jnp.where(lane == row + half, ends, strict)], axis=0)
    full_row = lax.broadcasted_iota(jnp.int32, (width, width), 0)
    full_lane = lax.broadcasted_iota(jnp.int32, (width, width), 1)
    return one_side + jnp.where(full_row == full_lane, 0.0, one_side.T)


def column(row):
    count = row.shape[1]
    spread = jnp.broadcast_to(row, (count, count))
    same = lax.broadcasted_iota(jnp.int32, (count, count), 0) == lax.broadcasted_iota(
        jnp.int32, (count, count), 1
    )
    picked = jnp.where(same, spread, 0).astype(F32)
    return jnp.sum(picked, axis=1, keepdims=True).astype(jnp.int32)


def partner(index, count, step):
    if count & (count - 1):
        return lax.rem(index + step, count)
    result = 0
    bit = 1
    while bit < count:
        held = lax.rem(lax.div(index, bit), 2)
        result = result + bit * ((1 - held) if step & bit else held)
        bit *= 2
    return result


def kernel(
    n_dp, n_mp, heads,
    ql_in, kl_in, qg_in, kg_in, qh_in, kh_in, qp_in, kp_in, qw_in, kw_in, qm_in, km_in,
    qw_out, kw_out, qm_out, km_out, mix, shrink_out,
    ql_ref, kl_ref, qg_ref, kg_ref, qh_ref, kh_ref, qp_ref, kp_ref, qw_ref, kw_ref, qm_ref, km_ref, in_sems,
    near_send, near_recv, own, far_recv, peak_send, peak_recv, peak2_send, peak2_recv,
    grams, gram_recv, row_send, row_recv,
    ns_s, ns_r, fs_s, fs_r, pk_s, pk_r, pm_s, pm_r, g_s, g_r, y_s, y_r, m_s, m_r,
):
    dp = lax.axis_index("dp")
    mp = lax.axis_index("mp")
    n_outer = n_dp // 2
    outer = lax.div(dp, 2)
    inner = lax.rem(dp, 2)
    core = lax.rem(mp, 2)
    group = lax.div(mp, 2)
    n_group = n_mp // 2
    q_rows = qm_ref.shape[1]
    k_rows = km_ref.shape[1]
    width = qm_ref.shape[2]
    tokens = qg_ref.shape[0]
    other_core = mp + 1 - 2 * core

    loads = [
        pltpu.make_async_copy(src, dst, in_sems.at[i])
        for i, (src, dst) in enumerate((
            (ql_in, ql_ref), (kl_in, kl_ref), (qg_in, qg_ref), (kg_in, kg_ref),
            (qp_in, qp_ref), (kp_in, kp_ref), (qh_in, qh_ref), (kh_in, kh_ref),
            (qm_in, qm_ref), (km_in, km_ref), (qw_in, qw_ref), (kw_in, kw_ref),
        ))
    ]
    for each in loads:
        each.start()

    barrier = pltpu.get_barrier_semaphore()
    for step in range(1, n_dp):
        pl.semaphore_signal(
            barrier, inc=1, device_id=(lax.rem(dp + step, n_dp), mp), device_id_type=MESH
        )
    def owner(step):
        across = lax.rem(dp + (step // n_group) * heads, n_dp)
        return across, 2 * lax.rem(group + step, n_group) + core

    for step in range(n_group + 1, 2 * n_group):
        pl.semaphore_signal(barrier, inc=1, device_id=owner(step), device_id_type=MESH)
    for step in range(1, n_mp):
        pl.semaphore_signal(
            barrier, inc=1, device_id=(dp, lax.rem(mp + step, n_mp)), device_id_type=MESH
        )

    def copy(src, dst, send, recv, where):
        return pltpu.make_async_remote_copy(
            src_ref=src, dst_ref=dst, send_sem=send, recv_sem=recv,
            device_id=where, device_id_type=MESH,
        )

    def term(dst, where, to_outer, to_inner):
        slot = 2 * to_outer + to_inner
        half = lax.div(slot, heads)
        cols = pl.ds(pl.multiple_of(lax.rem(slot, heads) * width, width), width)
        dst[where, :q_rows, :] = mm(ql_ref[half], qg_ref[:, cols])
        dst[where, q_rows:, :] = mm(kl_ref[half], kg_ref[:, cols])

    for each in loads[:4]:
        each.wait()
    order = list(range(n_outer - 1, -1, -1))
    neighbour = (dp + 1 - 2 * inner, mp)
    near = []
    for spot, step in enumerate(order):
        term(near_send, spot, partner(outer, n_outer, step), 1 - inner)
        if spot == 0:
            pl.semaphore_wait(barrier, n_dp + n_mp + n_group - 3)
        each = copy(near_send.at[spot], near_recv.at[spot], ns_s.at[spot], ns_r.at[spot], neighbour)
        each.start()
        near.append(each)

    for each in loads[4:8]:
        each.wait()
    local_heads = qp_ref.shape[0]
    lane = lax.broadcasted_iota(jnp.int32, (8, width), 1)
    peaks = jnp.full((8, width), LOWEST, F32)
    ids = lax.broadcasted_iota(jnp.int32, (qp_ref.shape[2], tokens), 1)
    for head in range(local_heads):
        span = slice(head * width, (head + 1) * width)
        pick_q = (ids == column(qp_ref[head])).astype(F32).astype(BF16)
        pick_k = (ids == column(kp_ref[head])).astype(F32).astype(BF16)
        score = jnp.sum(
            mm(pick_q, qh_ref[:, span]) * mm(pick_k, kh_ref[:, span]), axis=1, keepdims=True
        )
        top = jnp.max(score * SCORE_SCALE, axis=0, keepdims=True)
        peaks = jnp.where(lane == mp * local_heads + head, top, peaks)
    peak_send[...] = peaks
    peak_copies = []
    for step in range(1, n_dp):
        each = copy(
            peak_send, peak_recv.at[step - 1], pk_s.at[step - 1], pk_r.at[step - 1],
            (lax.rem(dp + step, n_dp), mp),
        )
        each.start()
        peak_copies.append(each)

    for spot, step in enumerate(order):
        term(own, spot, partner(outer, n_outer, step), inner)
    last = n_outer - 1
    relayed = n_outer == 4
    inside = lax.rem(lax.div(outer, 2) + lax.rem(outer, 2), 2)
    far = []
    for spot, step in enumerate(order):
        near[spot].wait_recv()
        if not step:
            continue
        own[spot] = own[spot] + near_recv[spot]
        where = spot
        target = partner(outer, n_outer, step)
        if relayed and spot == 0:
            where = last * (1 - inside)
            aside = partner(outer, n_outer, 1)
            target = aside + inside * (target - aside)
        if relayed and spot == 1:

            @pl.when(inside == 1)
            def _():
                copy(
                    own.at[0], far_recv.at[last], fs_s.at[0], fs_r.at[last], (dp, mp)
                ).wait_recv()
                own[1] = own[1] + far_recv[last]

        each = copy(
            own.at[spot], far_recv.at[where], fs_s.at[spot], fs_r.at[where],
            (2 * target + inner, mp),
        )
        each.start()
        far.append(each)
    own[last] = own[last] + near_recv[last]

    for each in peak_copies:
        each.wait_recv()
    peaks = jnp.maximum(peaks, jnp.max(peak_recv[...], axis=0))
    peak2_send[...] = peaks
    peak2_copies = []
    for step in range(1, n_mp):
        each = copy(
            peak2_send, peak2_recv.at[step - 1], pm_s.at[step - 1], pm_r.at[step - 1],
            (dp, lax.rem(mp + step, n_mp)),
        )
        each.start()
        peak2_copies.append(each)

    if relayed:

        @pl.when(inside == 1)
        def _():
            copy(own.at[0], far_recv.at[0], fs_s.at[0], fs_r.at[0], (dp, mp)).wait_recv()
            own[last] = own[last] + far_recv[0]

    total = own[last]
    for spot in range(1 if relayed else 0, last):
        far[spot].wait_recv()
        total = total + far_recv[spot]
    for each in loads[8:]:
        each.wait()
    q_moment = MOMENTUM * qm_ref[0] + total[:q_rows]
    k_moment = MOMENTUM * km_ref[0] + total[q_rows:]
    qm_out[0] = q_moment
    km_out[0] = k_moment

    top = width // 2
    for which, matrix in enumerate((gram(q_moment), gram(k_moment))):
        body, ends = fold(matrix)
        grams[which, :top, :] = body
        grams[which, top:, :] = ends
    swap = copy(grams.at[1 - core], gram_recv, g_s, g_r, (dp, other_core))
    swap.start()
    swap.wait_recv()
    whole = grams[core] + gram_recv[...]
    row_send[...] = whole
    rows = []
    for step in range(1, 2 * n_group):
        each = copy(
            row_send, row_recv.at[step - 1], y_s.at[step - 1], y_r.at[step - 1], owner(step)
        )
        each.start()
        rows.append(each)
    for each in peak2_copies:
        each.wait_recv()
    peaks = jnp.maximum(peaks, jnp.max(peak2_recv[...], axis=0))
    mine = jnp.where(lane == lax.rem(dp, heads), peaks, LOWEST)
    peak = jnp.max(jnp.max(mine, axis=0, keepdims=True), axis=1, keepdims=True)
    shrink = jnp.sqrt(CLIP_LEVEL / jnp.maximum(peak, CLIP_LEVEL))
    keep = 1.0 - STEP_SIZE * DECAY
    shrink_out[...] = jnp.broadcast_to(shrink, shrink_out.shape)
    qw_out[0] = (qw_ref[0] * keep) * shrink
    kw_out[0] = (kw_ref[0] * keep) * shrink
    for each in rows:
        each.wait_recv()
    whole = unfold(whole + jnp.sum(row_recv[...], axis=0))

    eye = (
        lax.broadcasted_iota(jnp.int32, (width, width), 0)
        == lax.broadcasted_iota(jnp.int32, (width, width), 1)
    ).astype(F32)
    trace = jnp.sum(jnp.sum(whole * eye, axis=0, keepdims=True), axis=1, keepdims=True)
    scale = 1.0 / jnp.sqrt(trace + 1.0)
    current = whole * (scale * scale)
    mixed = None
    for step in range(ITERS):
        parts = split(current)
        square = mm3(parts, parts)
        poly = COEFF_A * eye + COEFF_B * current + COEFF_C * square
        pair = split(poly)
        mixed = poly * scale if mixed is None else mm3(split(mixed), pair)
        if step + 1 < ITERS:
            current = mm3(split(mm3(parts, pair)), pair)
    mix[core] = mixed
    swap2 = copy(mix.at[core], mix.at[core], m_s, m_r, (dp, other_core))
    swap2.start()

    swap2.wait_recv()
    for each in near + far + peak_copies + peak2_copies + [swap] + rows + [swap2]:
        each.wait_send()


def finish(n_mp, qw_ref, kw_ref, qm_ref, km_ref, mix_ref, shrink_ref, qw_out, kw_out, qm_out, km_out):
    groups = ((qw_ref, qm_ref, qw_out, qm_out), (kw_ref, km_ref, kw_out, km_out))
    for which, (weight, moment, weight_out, moment_out) in enumerate(groups):
        rows = moment[0]
        size = STEP_SIZE * 0.2 * math.sqrt(2 * n_mp * rows.shape[0])
        ortho = mm3(split(rows), split(mix_ref[which]))
        moment_out[0] = rows
        weight_out[0] = weight[0] - (size * ortho) * shrink_ref[0:1, :]


def local(
    q_latent, kv_latent, q_head_grad, k_head_grad, q_heads, k_heads,
    query_pick, key_pick, q_weight, k_weight, q_moment, k_moment,
):
    n_dp = lax.axis_size("dp")
    n_mp = lax.axis_size("mp")
    heads = n_dp // 2
    n_outer = n_dp // 2
    n_group = n_mp // 2
    rows = q_latent.shape[2] + kv_latent.shape[2]
    width = q_moment.shape[2]
    operands = (
        q_latent.transpose(1, 2, 0), kv_latent.transpose(1, 2, 0), q_head_grad, k_head_grad,
        q_heads, k_heads, query_pick.transpose(2, 0, 1), key_pick.transpose(2, 0, 1),
        q_weight, k_weight, q_moment, k_moment,
    )
    vmem = pltpu.VMEM
    dma = pltpu.SemaphoreType.DMA
    square = (width, width)
    folded = (width // 2 + 8, width)
    tile = (8, width)
    shapes = [a.shape for a in (q_weight, k_weight, q_moment, k_moment)]
    parts = pl.pallas_call(
        functools.partial(kernel, n_dp, n_mp, heads),
        out_shape=[vmem(shape, F32) for shape in shapes + [(2,) + square, tile]],
        in_specs=[pl.BlockSpec(memory_space=pl.ANY)] * 12,
        out_specs=[pl.BlockSpec(memory_space=vmem)] * 6,
        scratch_shapes=[vmem(a.shape, a.dtype) for a in operands] + [
            dma((12,)),
            vmem((n_outer, rows, width), F32),
            vmem((n_outer, rows, width), F32),
            vmem((n_outer, rows, width), F32),
            vmem((n_outer, rows, width), F32),
            vmem(tile, F32),
            vmem((n_dp - 1,) + tile, F32),
            vmem(tile, F32),
            vmem((n_mp - 1,) + tile, F32),
            vmem((2,) + folded, F32),
            vmem(folded, F32),
            vmem(folded, F32),
            vmem((2 * n_group - 1,) + folded, F32),
            dma((n_outer,)), dma((n_outer,)),
            dma((n_outer,)), dma((n_outer,)),
            dma((n_dp - 1,)), dma((n_dp - 1,)),
            dma((n_mp - 1,)), dma((n_mp - 1,)),
            dma, dma,
            dma((2 * n_group - 1,)), dma((2 * n_group - 1,)),
            dma, dma,
        ],
        compiler_params=pltpu.CompilerParams(
            collective_id=0, has_side_effects=True, vmem_limit_bytes=56 * 1024 * 1024
        ),
    )(*operands)
    return pl.pallas_call(
        functools.partial(finish, n_mp),
        out_shape=[jax.ShapeDtypeStruct(shape, F32) for shape in shapes],
        in_specs=[pl.BlockSpec(memory_space=vmem)] * 6,
        out_specs=[pl.BlockSpec(memory_space=vmem)] * 4,
    )(*[pltpu.with_memory_space_constraint(part, vmem) for part in parts])


def solution(mesh):
    rows3 = P("dp", "mp", None)
    in_specs = (
        P("dp", None, "mp"), P("dp", None, "mp"), P("dp", None), P("dp", None),
        P("dp", "mp"), P("dp", "mp"), P("dp", None, "mp"), P("dp", None, "mp"),
        rows3, rows3, rows3, rows3,
    )
    return jax.shard_map(
        lambda *args: tuple(local(*args)),
        mesh=mesh, in_specs=in_specs, out_specs=(rows3,) * 4, check_vma=False,
    )
```
